128 devices in a mesh: dap: 128 (over x, y, z, core).
Axes of the slice: x: 4, y: 4, z: 4, core: 2. Of those that a mesh axis runs over, the one named last changes fastest.
Arguments:
- pair: bfloat16 [512, 512, 128], P('dap'), may hold values from -6 to 6
- residue_mask: int32 [512], P('dap'), may hold values 0 or 1
- norm_gain: float32 [2, 128], replicated, may hold values from 0.5 to 1.5
- proj_weight: bfloat16 [2, 128, 512], replicated, may hold values from -0.5 to 0.5
- gate_weight: bfloat16 [2, 128, 128], replicated, may hold values from -0.5 to 0.5
- mix_gain: float32 [2, 128], replicated, may hold values from 0.5 to 1.5
- out_weight: bfloat16 [2, 128, 128], replicated, may hold values from -0.5 to 0.5
Outputs:
- updated_pair: bfloat16 [512, 512, 128], P('dap')
The draws below stay inside these ranges and needn't reach their ends.
All inputs are finite; a program needn't handle non-finite values. No bound on the sum of `residue_mask` on one device may be relied on, other than what follows from the above.
Results may differ from the reference program's by a relative error of at most 0.0061.
Values may be sent and summed in bfloat16 or wider, within the bound.
A program may use at most 64 MiB of HBM per device.

```python
import jax
import jax.numpy as jnp
from jax import lax

C = 128
H = 128
ROWS = 4
N = 512
N_DAP = 128


def place_ends(result, own_key, smallest, largest):
    extent = result.shape
    spot = [jax.random.randint(jax.random.fold_in(own_key, axis), (), 0, extent[axis]) for axis in range(len(extent))]
    result = result.at[tuple(spot)].set(smallest)
    longest = extent.index(max(extent))
    spot[longest] = (spot[longest] + 1) % extent[longest]
    return result.at[tuple(spot)].set(largest)


def shard_levels(own_key, dims, pieces, smallest, high):
    level = 1.0
    for axis_at, blocks in pieces:
        heights = jax.random.uniform(jax.random.fold_in(jax.random.fold_in(own_key, 6), axis_at), (blocks,), jnp.float32, smallest / len(pieces), high / len(pieces))
        level = level * jnp.repeat(jnp.exp(heights), dims[axis_at] // blocks).reshape((-1,) + (1,) * (len(dims) - 1 - axis_at))
    return level


def noise(stream_key, dims, scale, bound, pieces=(), dtype=jnp.bfloat16):
    result = jax.random.normal(stream_key, dims, jnp.float32) * scale
    if len(pieces) > 0:
        result = shard_levels(stream_key, dims, pieces, -0.22, 0.18) * result
    return jnp.clip(result, min=-bound, max=bound).astype(dtype)


def setup_inputs(seed: int = 0) -> dict:
    key_list = jax.random.split(jax.random.key(seed), 8)
    return {
        "pair": noise(key_list[0], (N, N, C), 1.0, 6.0, ((0, 128),)),
        "residue_mask": place_ends((jax.random.randint(key_list[1], (N,), 0, 4) < 3).astype(jnp.int32), jax.random.fold_in(key_list[1], 1), 0, 1),
        "norm_gain": jnp.clip(jax.random.uniform(key_list[2], (2, C), jnp.float32, 0.5, 1.5), 0.5, 1.5),
        "proj_weight": noise(key_list[3], (2, C, 4 * H), C ** -0.5, 0.5),
        "gate_weight": noise(key_list[4], (2, C, C), C ** -0.5, 0.5),
        "mix_gain": jnp.clip(jax.random.uniform(key_list[5], (2, H), jnp.float32, 0.5, 1.5), 0.5, 1.5),
        "out_weight": noise(key_list[6], (2, H, C), H ** -0.5, 0.5),
    }


EPS = 1e-05

def normalize(values, axis):
    center = values - lax.optimization_barrier(jnp.mean(values, axis=axis, keepdims=True))
    spread = lax.optimization_barrier(jnp.mean(center * center, axis=axis, keepdims=True))
    return center * lax.rsqrt(spread + EPS)

def norm_rows(rows, gain):
    return (normalize(rows.astype(jnp.float32), 2) * gain).astype(jnp.bfloat16)

def panels(normed, mask_rows, mask_all, weight):
    proj = jnp.einsum('rnc,ch->hrn', normed.astype(jnp.float32), weight.astype(jnp.float32))
    hidden = weight.shape[1] // 4
    scale = mask_rows.astype(jnp.float32)[:, None] * mask_all.astype(jnp.float32)[None, :]
    left = (jax.nn.sigmoid(proj[:hidden]) * proj[hidden:2 * hidden] * scale).astype(jnp.bfloat16)
    right = (jax.nn.sigmoid(proj[2 * hidden:3 * hidden]) * proj[3 * hidden:] * scale).astype(jnp.bfloat16)
    return (left, right)

def finish(rows, normed, tri_rows, gate_w, tri_gain, out_w):
    gate = jax.nn.sigmoid(jnp.einsum('rnc,cd->rnd', normed.astype(jnp.float32), gate_w.astype(jnp.float32)))
    tri_normed = (normalize(tri_rows.astype(jnp.float32), 0) * tri_gain[:, None, None]).astype(jnp.bfloat16)
    out = jnp.einsum('hrn,hc->rnc', tri_normed.astype(jnp.float32), out_w.astype(jnp.float32))
    return (rows.astype(jnp.float32) + gate * out).astype(jnp.bfloat16)

def reference(pair, residue_mask, norm_gain, proj_weight, gate_weight, mix_gain, out_weight):
    total = pair.shape[0]
    chans = pair.shape[2]
    hidden = proj_weight.shape[2] // 4
    mask_blocks = residue_mask.reshape(N_DAP, ROWS)
    z = pair
    for layer in range(2):
        blocks = z.reshape(N_DAP, ROWS, total, chans)

        def make(args):
            rows, mrows = args
            normed = norm_rows(rows, norm_gain[layer])
            return panels(normed, mrows, residue_mask, proj_weight[layer])
        left, right = lax.map(make, (blocks, mask_blocks))
        left = left.transpose(1, 0, 2, 3).reshape(hidden, total, total)
        right = right.transpose(1, 0, 2, 3).reshape(hidden, total, total)

        def channel(args):
            one, two = args
            one = one.astype(jnp.float32)
            two = two.astype(jnp.float32)
            if layer == 0:
                prod = jnp.dot(one, two.T)
            else:
                prod = jnp.dot(one.T, two)
            return prod.astype(jnp.bfloat16)
        tri = lax.map(channel, (left, right))
        tri_blocks = tri.reshape(hidden, N_DAP, ROWS, total).transpose(1, 0, 2, 3)

        def close(args):
            rows, tri_rows = args
            normed = norm_rows(rows, norm_gain[layer])
            return finish(rows, normed, tri_rows, gate_weight[layer], mix_gain[layer], out_weight[layer])
        z = lax.map(close, (blocks, tri_blocks)).reshape(total, total, chans)
    return z
```

```python
import functools

import jax
import jax.numpy as jnp
from jax import lax
from jax.experimental import pallas as pl
from jax.experimental.pallas import tpu as pltpu
from jax.sharding import PartitionSpec as P

EPS = 1e-05
ND = 128
MESH = pl.DeviceIdType.MESH
F32 = jnp.float32
BF16 = jnp.bfloat16


def offset_order():
    offs = [(a, b, c, d) for a in range(4) for b in range(4) for c in range(4) for d in range(2)][1:]
    offs.sort(key=lambda o: -sum(min(v, 4 - v) for v in o[:3]))
    groups = {}
    for o in offs:
        key = next(((a, o[a]) for a in range(3) if o[a]), (3, 0))
        groups.setdefault(key, []).append(o)
    timed = [((i + 0.5) / len(g), o) for g in groups.values() for i, o in enumerate(g)]
    timed.sort(key=lambda t: t[0])
    return [o for _, o in timed]


ORDER = offset_order()


def sigmoid(v):
    return 0.5 * jnp.tanh(0.5 * v) + 0.5


def normalize(v):
    center = v - jnp.mean(v, axis=0, keepdims=True)
    spread = jnp.mean(center * center, axis=0, keepdims=True)
    return center * lax.rsqrt(spread + EPS)


def kernel(
    pair, mask, norm_gain, proj_w, gate_w, mix_gain, out_w, out,
    xt, nt, wt, gwt, owt, gains, flat, send, recv, tsend, trecv, mat_a, mat_b, msend, mrecv, mrow,
    ssem, rsem,
):
    me = lax.axis_index("dap")
    core, z = lax.rem(me, 2), lax.rem(me // 2, 4)
    y, x = lax.rem(me // 8, 4), me // 32
    xs = [lax.rem(x + d, 4) * 32 for d in range(4)]
    ys = [lax.rem(y + d, 4) * 8 for d in range(4)]
    zs = [lax.rem(z + d, 4) * 2 for d in range(4)]
    cs = [lax.rem(core + d, 2) for d in range(2)]
    peers = [xs[a] + ys[b] + zs[c] + cs[d] for a, b, c, d in ORDER]

    barrier = pltpu.get_barrier_semaphore()
    for peer in peers:
        pl.semaphore_signal(barrier, inc=1, device_id=(peer,), device_id_type=MESH)

    for u in range(2):
        wt[u] = proj_w[u].astype(F32).T.astype(BF16)
        gwt[u] = gate_w[u].astype(F32).T.astype(BF16)
        owt[u] = out_w[u].astype(F32).T.astype(BF16)
        gains[0, u] = jnp.broadcast_to(norm_gain[u : u + 1, :], (128, 128)).T
        gains[1, u] = jnp.broadcast_to(mix_gain[u : u + 1, :], (128, 128)).T

    lane = lax.broadcasted_iota(jnp.int32, (1, 128), 1)
    base = lax.rem(me, 32) * 4
    row = jnp.zeros((1, 128), F32)
    for r in range(4):
        row = jnp.where(lane == base + r, mask[0, r].astype(F32), row)
    msend[...] = row

    def load_pair(s, _):
        at = pl.multiple_of(s * 128, 128)
        xt[:, pl.ds(at, 128)] = pair[s // 4, pl.ds(pl.multiple_of(lax.rem(s, 4) * 128, 128), 128), :].astype(F32).T
        return 0

    lax.fori_loop(0, 16, load_pair, 0)

    def panel_step(u, s):
        at = pl.multiple_of(s * 128, 128)
        normed = (normalize(xt[:, pl.ds(at, 128)]) * gains[0, u]).astype(BF16)
        nt[:, pl.ds(at, 128)] = normed
        keep = mask[0, s // 4].astype(F32)
        if u == 1:
            keep = keep * mrow[pl.ds(lax.rem(s, 4), 1), :]
        for p in range(2):
            proj = jnp.dot(wt[u, p * 256 : p * 256 + 256, :], normed, preferred_element_type=F32)
            flat[p, pl.ds(s, 128, stride=16), :] = sigmoid(proj[:128]) * proj[128:] * keep

    def pack(u):
        def step(c, _):
            for p in range(2):
                rows = flat[p, pl.ds(pl.multiple_of(c * 128, 128), 128), :]
                send[u, pl.ds(c * 8, 8), p] = rows.astype(BF16).reshape(8, 16, 128)
            return 0

        lax.fori_loop(0, 16, step, 0)

    def exchange(k, src, dst):
        for peer in peers:
            pltpu.make_async_remote_copy(
                src.at[peer], dst.at[me], ssem.at[k], rsem.at[k], device_id=(peer,), device_id_type=MESH
            ).start()
        dst[me] = src[me]

    def arrived(k, dst):
        part = dst.at[pl.ds(0, ND - 1)]
        pltpu.make_async_copy(part, part, rsem.at[k]).wait()

    def sent(k, src):
        part = src.at[pl.ds(0, ND - 1)]
        pltpu.make_async_copy(part, part, ssem.at[k]).wait()

    def products(u):
        def spread(d, _):
            for p in range(2):
                rows = recv[u, pl.ds(d * 8, 8), p].reshape(128, 128).astype(F32)
                flat[p, pl.ds(pl.multiple_of(d * 128, 128), 128), :] = rows
            return 0

        lax.fori_loop(0, 16, spread, 0)
        for q in range(4):
            left = flat[0, pl.ds(q, 512, stride=4), :]
            right = flat[1, pl.ds(q, 512, stride=4), :]
            if u == 0:
                mat_a[:, q * 128 : q * 128 + 128] = (left * mrow[q : q + 1, :]).astype(BF16)
            else:
                mat_a[q * 128 : q * 128 + 128, :] = left.T.astype(BF16)
            mat_b[:, q * 128 : q * 128 + 128] = right.astype(BF16)
        for q in range(4):
            if u == 0:
                tri = lax.dot_general(
                    mat_a[...], mat_b[q * 128 : q * 128 + 128, :], (((1,), (1,)), ((), ())), preferred_element_type=F32
                )
            else:
                tri = jnp.dot(mat_a[...], mat_b[:, q * 128 : q * 128 + 128], preferred_element_type=F32)
            flat[0, pl.ds(q, 512, stride=4), :] = tri

        def gather(d, _):
            rows = flat[0, pl.ds(pl.multiple_of(d * 128, 128), 128), :]
            tsend[u, pl.ds(d * 8, 8)] = rows.astype(BF16).reshape(8, 16, 128)
            return 0

        lax.fori_loop(0, 16, gather, 0)

    def unpack(u):
        def step(c, _):
            rows = trecv[u, pl.ds(c * 8, 8)].reshape(128, 128).astype(F32)
            flat[0, pl.ds(pl.multiple_of(c * 128, 128), 128), :] = rows
            return 0

        lax.fori_loop(0, 16, step, 0)

    def finish_step(u, s):
        at = pl.multiple_of(s * 128, 128)
        tri = flat[0, pl.ds(s, 128, stride=16), :]
        normed = (normalize(tri) * gains[1, u]).astype(BF16)
        result = jnp.dot(owt[u], normed, preferred_element_type=F32)
        gate = sigmoid(jnp.dot(gwt[u], nt[:, pl.ds(at, 128)], preferred_element_type=F32))
        return at, (xt[:, pl.ds(at, 128)] + gate * result).astype(BF16).astype(F32)

    def first_panels(s, _):
        panel_step(0, s)
        return 0

    lax.fori_loop(0, 16, first_panels, 0)
    pack(0)
    pl.semaphore_wait(barrier, ND - 1)
    for peer in peers:
        pltpu.make_async_remote_copy(
            msend, mrecv.at[me], ssem.at[4], rsem.at[4], device_id=(peer,), device_id_type=MESH
        ).start()
    mrecv[me] = msend[...]
    exchange(0, send.at[0], recv.at[0])
    arrived(4, mrecv)
    for q in range(4):
        mrow[q : q + 1, :] = jnp.sum(mrecv[q * 32 : q * 32 + 32], axis=0)
    arrived(0, recv.at[0])
    products(0)
    exchange(1, tsend.at[0], trecv.at[0])
    arrived(1, trecv.at[0])
    unpack(0)

    def middle(s, _):
        at, value = finish_step(0, s)
        xt[:, pl.ds(at, 128)] = value
        return 0

    lax.fori_loop(0, 16, middle, 0)

    def second_panels(s, _):
        panel_step(1, s)
        return 0

    lax.fori_loop(0, 16, second_panels, 0)
    pack(1)
    exchange(2, send.at[1], recv.at[1])
    arrived(2, recv.at[1])
    products(1)
    exchange(3, tsend.at[1], trecv.at[1])
    arrived(3, trecv.at[1])
    unpack(1)

    def last(s, _):
        _, value = finish_step(1, s)
        out[s // 4, pl.ds(pl.multiple_of(lax.rem(s, 4) * 128, 128), 128), :] = value.T.astype(BF16)
        return 0

    lax.fori_loop(0, 16, last, 0)
    sent(4, mrecv)
    sent(0, send.at[0])
    sent(1, tsend.at[0])
    sent(2, send.at[1])
    sent(3, tsend.at[1])


def body(pair, residue_mask, norm_gain, proj_weight, gate_weight, mix_gain, out_weight):
    vmem = pl.BlockSpec(memory_space=pltpu.VMEM)
    return pl.pallas_call(
        kernel,
        out_shape=jax.ShapeDtypeStruct((4, 512, 128), BF16),
        in_specs=[vmem, pl.BlockSpec(memory_space=pltpu.SMEM)] + [vmem] * 5,
        out_specs=vmem,
        scratch_shapes=[
            pltpu.VMEM((128, 2048), F32),
            pltpu.VMEM((128, 2048), BF16),
            pltpu.VMEM((2, 512, 128), BF16),
            pltpu.VMEM((2, 128, 128), BF16),
            pltpu.VMEM((2, 128, 128), BF16),
            pltpu.VMEM((2, 2, 128, 128), F32),
            pltpu.VMEM((2, 2048, 128), F32),
            pltpu.VMEM((2, ND, 2, 16, 128), BF16),
            pltpu.VMEM((2, ND, 2, 16, 128), BF16),
            pltpu.VMEM((2, ND, 16, 128), BF16),
            pltpu.VMEM((2, ND, 16, 128), BF16),
            pltpu.VMEM((512, 512), BF16),
            pltpu.VMEM((512, 512), BF16),
            pltpu.VMEM((1, 128), F32),
            pltpu.VMEM((ND, 1, 128), F32),
            pltpu.VMEM((4, 128), F32),
            pltpu.SemaphoreType.DMA((5,)),
            pltpu.SemaphoreType.DMA((5,)),
        ],
        compiler_params=pltpu.CompilerParams(collective_id=0, has_side_effects=True, vmem_limit_bytes=48 << 20),
    )(pair, residue_mask.reshape(1, 4), norm_gain, proj_weight, gate_weight, mix_gain, out_weight)


def solution(mesh):
    in_specs = (P("dap", None, None), P("dap"), P(), P(), P(), P(), P())
    return jax.shard_map(body, mesh=mesh, in_specs=in_specs, out_specs=P("dap", None, None), check_vma=False)
```

```python
import functools

import jax
import jax.numpy as jnp
from jax import lax
from jax.experimental import pallas as pl
from jax.experimental.pallas import tpu as pltpu
from jax.sharding import PartitionSpec as P

EPS = 1e-05
ND = 128
MESH = pl.DeviceIdType.MESH
F32 = jnp.float32
BF16 = jnp.bfloat16


def offset_order():
    offs = [(a, b, c, d) for a in range(4) for b in range(4) for c in range(4) for d in range(2)][1:]
    offs.sort(key=lambda o: -sum(min(v, 4 - v) for v in o[:3]))
    groups = {}
    for o in offs:
        key = next(((a, o[a]) for a in range(3) if o[a]), (3, 0))
        groups.setdefault(key, []).append(o)
    timed = [((i + 0.5) / len(g), o) for g in groups.values() for i, o in enumerate(g)]
    timed.sort(key=lambda t: t[0])
    return [o for _, o in timed]


ORDER = offset_order()


def sigmoid(v):
    return 0.5 * jnp.tanh(0.5 * v) + 0.5


def normalize(v):
    center = v - jnp.mean(v, axis=0, keepdims=True)
    spread = jnp.mean(center * center, axis=0, keepdims=True)
    return center * lax.rsqrt(spread + EPS)


def kernel(
    pair_h, mask, norm_gain_h, proj_w_h, gate_w_h, mix_gain_h, out_w_h, out,
    pair, norm_gain, proj_w, gate_w, mix_gain, out_w, isem, xt, nt, wt, gwt, owt, gains, flat, send, recv, tsend, trecv, mat_a, mat_b, msend, mrecv, mrow,
    ssem, rsem,
):
    pairs = (
        (pair_h, pair), (norm_gain_h, norm_gain), (proj_w_h, proj_w),
        (gate_w_h, gate_w), (mix_gain_h, mix_gain), (out_w_h, out_w),
    )
    loads = [pltpu.make_async_copy(a, b, isem.at[i]) for i, (a, b) in enumerate(pairs)]
    for load in loads:
        load.start()
    me = lax.axis_index("dap")
    core, z = lax.rem(me, 2), lax.rem(me // 2, 4)
    y, x = lax.rem(me // 8, 4), me // 32
    xs = [lax.rem(x + d, 4) * 32 for d in range(4)]
    ys = [lax.rem(y + d, 4) * 8 for d in range(4)]
    zs = [lax.rem(z + d, 4) * 2 for d in range(4)]
    cs = [lax.rem(core + d, 2) for d in range(2)]
    peers = [xs[a] + ys[b] + zs[c] + cs[d] for a, b, c, d in ORDER]

    barrier = pltpu.get_barrier_semaphore()
    for peer in peers:
        pl.semaphore_signal(barrier, inc=1, device_id=(peer,), device_id_type=MESH)

    for load in loads:
        load.wait()
    for u in range(2):
        wt[u] = proj_w[u].astype(F32).T.astype(BF16)
        gwt[u] = gate_w[u].astype(F32).T.astype(BF16)
        owt[u] = out_w[u].astype(F32).T.astype(BF16)
        gains[0, u] = jnp.broadcast_to(norm_gain[u : u + 1, :], (128, 128)).T
        gains[1, u] = jnp.broadcast_to(mix_gain[u : u + 1, :], (128, 128)).T

    lane = lax.broadcasted_iota(jnp.int32, (1, 128), 1)
    base = lax.rem(me, 32) * 4
    row = jnp.zeros((1, 128), F32)
    for r in range(4):
        row = jnp.where(lane == base + r, mask[0, r].astype(F32), row)
    msend[...] = row

    for r in range(4):
        xt[:, r * 512 : r * 512 + 512] = pair[r].astype(F32).T

    def tiled(column, times):
        return jnp.concatenate([column] * times, axis=1)

    def panels(u):
        for r in range(4):
            at = slice(r * 512, r * 512 + 512)
            normed = (normalize(xt[:, at]) * tiled(gains[0, u], 4)).astype(BF16)
            nt[:, at] = normed
            keep = mask[0, r].astype(F32)
            if u == 1:
                keep = keep * jnp.concatenate([mrow[q : q + 1, :] for q in range(4)], axis=1)
            for p in range(2):
                proj = jnp.dot(wt[u, p * 256 : p * 256 + 256, :], normed, preferred_element_type=F32)
                value = sigmoid(proj[:128]) * proj[128:] * keep
                for q in range(4):
                    flat[p, pl.ds(r * 4 + q, 128, stride=16), :] = value[:, q * 128 : q * 128 + 128]

    def pack(u):
        def step(c, _):
            for p in range(2):
                rows = flat[p, pl.ds(pl.multiple_of(c * 128, 128), 128), :]
                send[u, pl.ds(c * 8, 8), p] = rows.astype(BF16).reshape(8, 16, 128)
            return 0

        lax.fori_loop(0, 16, step, 0)

    def exchange(k, src, dst):
        for peer in peers:
            pltpu.make_async_remote_copy(
                src.at[peer], dst.at[me], ssem.at[k], rsem.at[k], device_id=(peer,), device_id_type=MESH
            ).start()
        dst[me] = src[me]

    def arrived(k, dst):
        part = dst.at[pl.ds(0, ND - 1)]
        pltpu.make_async_copy(part, part, rsem.at[k]).wait()

    def sent(k, src):
        part = src.at[pl.ds(0, ND - 1)]
        pltpu.make_async_copy(part, part, ssem.at[k]).wait()

    def products(u):
        def spread(d, _):
            for p in range(2):
                rows = recv[u, pl.ds(d * 8, 8), p].reshape(128, 128).astype(F32)
                flat[p, pl.ds(pl.multiple_of(d * 128, 128), 128), :] = rows
            return 0

        lax.fori_loop(0, 16, spread, 0)
        for q in range(4):
            left = flat[0, pl.ds(q, 512, stride=4), :]
            right = flat[1, pl.ds(q, 512, stride=4), :]
            if u == 0:
                mat_a[:, q * 128 : q * 128 + 128] = (left * mrow[q : q + 1, :]).astype(BF16)
            else:
                mat_a[q * 128 : q * 128 + 128, :] = left.T.astype(BF16)
            mat_b[:, q * 128 : q * 128 + 128] = right.astype(BF16)
        for q in range(4):
            if u == 0:
                tri = lax.dot_general(
                    mat_a[...], mat_b[q * 128 : q * 128 + 128, :], (((1,), (1,)), ((), ())), preferred_element_type=F32
                )
            else:
                tri = jnp.dot(mat_a[...], mat_b[:, q * 128 : q * 128 + 128], preferred_element_type=F32)
            flat[0, pl.ds(q, 512, stride=4), :] = tri

        def gather(d, _):
            rows = flat[0, pl.ds(pl.multiple_of(d * 128, 128), 128), :]
            tsend[u, pl.ds(d * 8, 8)] = rows.astype(BF16).reshape(8, 16, 128)
            return 0

        lax.fori_loop(0, 16, gather, 0)

    def unpack(u):
        def step(c, _):
            rows = trecv[u, pl.ds(c * 8, 8)].reshape(128, 128).astype(F32)
            flat[0, pl.ds(pl.multiple_of(c * 128, 128), 128), :] = rows
            return 0

        lax.fori_loop(0, 16, step, 0)

    def finish(u, put):
        for r in range(4):
            at = slice(r * 512, r * 512 + 512)
            tri = jnp.concatenate([flat[0, pl.ds(r * 4 + q, 128, stride=16), :] for q in range(4)], axis=1)
            normed = (normalize(tri) * tiled(gains[1, u], 4)).astype(BF16)
            result = jnp.dot(owt[u], normed, preferred_element_type=F32)
            gate = sigmoid(jnp.dot(gwt[u], nt[:, at], preferred_element_type=F32))
            put(r, at, xt[:, at] + gate * result)

    panels(0)
    pack(0)
    pl.semaphore_wait(barrier, ND - 1)
    for peer in peers:
        pltpu.make_async_remote_copy(
            msend, mrecv.at[me], ssem.at[4], rsem.at[4], device_id=(peer,), device_id_type=MESH
        ).start()
    mrecv[me] = msend[...]
    exchange(0, send.at[0], recv.at[0])
    arrived(4, mrecv)
    for q in range(4):
        mrow[q : q + 1, :] = jnp.sum(mrecv[q * 32 : q * 32 + 32], axis=0)
    arrived(0, recv.at[0])
    products(0)
    exchange(1, tsend.at[0], trecv.at[0])
    arrived(1, trecv.at[0])
    unpack(0)

    def middle(r, at, value):
        xt[:, at] = value.astype(BF16).astype(F32)

    finish(0, middle)
    panels(1)
    pack(1)
    exchange(2, send.at[1], recv.at[1])
    arrived(2, recv.at[1])
    products(1)
    exchange(3, tsend.at[1], trecv.at[1])
    arrived(3, trecv.at[1])
    unpack(1)

    def last(r, at, value):
        out[r] = value.T.astype(BF16)

    finish(1, last)
    sent(4, mrecv)
    sent(0, send.at[0])
    sent(1, tsend.at[0])
    sent(2, send.at[1])
    sent(3, tsend.at[1])


def body(pair, residue_mask, norm_gain, proj_weight, gate_weight, mix_gain, out_weight):
    vmem, hbm = pl.BlockSpec(memory_space=pltpu.VMEM), pl.BlockSpec(memory_space=pltpu.HBM)
    return pl.pallas_call(
        kernel,
        out_shape=jax.ShapeDtypeStruct((4, 512, 128), BF16),
        in_specs=[hbm, pl.BlockSpec(memory_space=pltpu.SMEM)] + [hbm] * 5,
        out_specs=vmem,
        scratch_shapes=[
            pltpu.VMEM((4, 512, 128), BF16),
            pltpu.VMEM((2, 128), F32),
            pltpu.VMEM((2, 128, 512), BF16),
            pltpu.VMEM((2, 128, 128), BF16),
            pltpu.VMEM((2, 128), F32),
            pltpu.VMEM((2, 128, 128), BF16),
            pltpu.SemaphoreType.DMA((6,)),
            pltpu.VMEM((128, 2048), F32),
            pltpu.VMEM((128, 2048), BF16),
            pltpu.VMEM((2, 512, 128), BF16),
            pltpu.VMEM((2, 128, 128), BF16),
            pltpu.VMEM((2, 128, 128), BF16),
            pltpu.VMEM((2, 2, 128, 128), F32),
            pltpu.VMEM((2, 2048, 128), F32),
            pltpu.VMEM((2, ND, 2, 16, 128), BF16),
            pltpu.VMEM((2, ND, 2, 16, 128), BF16),
            pltpu.VMEM((2, ND, 16, 128), BF16),
            pltpu.VMEM((2, ND, 16, 128), BF16),
            pltpu.VMEM((512, 512), BF16),
            pltpu.VMEM((512, 512), BF16),
            pltpu.VMEM((1, 128), F32),
            pltpu.VMEM((ND, 1, 128), F32),
            pltpu.VMEM((4, 128), F32),
            pltpu.SemaphoreType.DMA((5,)),
            pltpu.SemaphoreType.DMA((5,)),
        ],
        compiler_params=pltpu.CompilerParams(collective_id=0, has_side_effects=True, vmem_limit_bytes=67_043_328),
    )(pair, residue_mask.reshape(1, 4), norm_gain, proj_weight, gate_weight, mix_gain, out_weight)


def solution(mesh):
    in_specs = (P("dap", None, None), P("dap"), P(), P(), P(), P(), P())
    return jax.shard_map(body, mesh=mesh, in_specs=in_specs, out_specs=P("dap", None, None), check_vma=False)
```

```python
import jax
import jax.numpy as jnp
from jax import lax
from jax.experimental import pallas as pl
from jax.experimental.pallas import tpu as pltpu
from jax.sharding import PartitionSpec as P

EPS = 1e-05
ND = 128
MESH = pl.DeviceIdType.MESH
F32 = jnp.float32
BF16 = jnp.bfloat16
R0, L0, T0, R1, L1, T1, MASK, KINDS = 0, 1, 5, 9, 13, 17, 21, 22


def sigmoid(v):
    return 0.5 * jnp.tanh(0.5 * v) + 0.5


def normalize(v):
    center = v - jnp.mean(v, axis=0, keepdims=True)
    spread = jnp.mean(center * center, axis=0, keepdims=True)
    return center * lax.rsqrt(spread + EPS)


def tiled(column):
    return jnp.concatenate([column] * 4, axis=1)


def offset_order():
    offs = [(a, b, c, d) for a in range(4) for b in range(4) for c in range(4) for d in range(2)][1:]
    offs.sort(key=lambda o: -sum(min(v, 4 - v) for v in o[:3]))
    groups = {}
    for o in offs:
        key = next(((a, o[a]) for a in range(3) if o[a]), (3, 0))
        groups.setdefault(key, []).append(o)
    timed = [((i + 0.5) / len(g), o) for g in groups.values() for i, o in enumerate(g)]
    timed.sort(key=lambda t: t[0])
    return [o for _, o in timed]


ORDER = offset_order()


def kernel(
    pair_h, mask, norm_gain_h, proj_w_h, gate_w_h, mix_gain_h, out_w_h, out_h,
    pair, norm_gain, proj_w, gate_w, mix_gain, out_w, isem,
    xt, nt, wt, gwt, owt, gains, flat, mat_a, mat_b, msend, mrecv, mrow,
    r0_send, r0_recv, l0_send, l0_recv, t0_send, t0_recv, r1_send, r1_recv, l1_send, l1_recv, t1_send, t1_recv,
    ssem, rsem,
):
    pairs = (
        (pair_h, pair), (proj_w_h, proj_w), (norm_gain_h, norm_gain),
        (gate_w_h, gate_w), (mix_gain_h, mix_gain), (out_w_h, out_w),
    )
    loads = [pltpu.make_async_copy(a, b, isem.at[i]) for i, (a, b) in enumerate(pairs)]
    for load in loads:
        load.start()
    me = lax.axis_index("dap")
    core, z = lax.rem(me, 2), lax.rem(me // 2, 4)
    y, x = lax.rem(me // 8, 4), me // 32
    xs = [lax.rem(x + d, 4) * 32 for d in range(4)]
    ys = [lax.rem(y + d, 4) * 8 for d in range(4)]
    zs = [lax.rem(z + d, 4) * 2 for d in range(4)]
    cs = [lax.rem(core + d, 2) for d in range(2)]
    peers = [xs[a] + ys[b] + zs[c] + cs[d] for a, b, c, d in ORDER]

    def to_all(send_one):
        for peer in peers:
            send_one(peer)

    barrier = pltpu.get_barrier_semaphore()
    to_all(lambda peer: pl.semaphore_signal(barrier, inc=1, device_id=(peer,), device_id_type=MESH))

    def exchange(k, src, dst):
        to_all(
            lambda peer: pltpu.make_async_remote_copy(
                src.at[peer], dst.at[me], ssem.at[k], rsem.at[k], device_id=(peer,), device_id_type=MESH
            ).start()
        )
        dst[me] = src[me]

    def arrived(k, dst):
        part = dst.at[pl.ds(0, ND - 1)]
        pltpu.make_async_copy(part, part, rsem.at[k]).wait()

    def sent(k, src):
        part = src.at[pl.ds(0, ND - 1)]
        pltpu.make_async_copy(part, part, ssem.at[k]).wait()

    def pack(base, rows, dst):
        per = 128 // rows
        for c in range(rows):
            dst[pl.ds(c * per, per)] = flat[pl.ds(base + c * 128, 128), :].astype(BF16).reshape(per, rows, 128)

    def unpack(base, rows, src):
        per = 128 // rows
        for c in range(rows):
            flat[pl.ds(base + c * 128, 128), :] = src[pl.ds(c * per, per)].reshape(128, 128).astype(F32)

    def prepare(u):
        wt[u] = proj_w[u].astype(F32).T.astype(BF16)
        gains[0, u] = jnp.broadcast_to(norm_gain[u : u + 1, :], (128, 128)).T

    def prepare_late(u):
        gwt[u] = gate_w[u].astype(F32).T.astype(BF16)
        owt[u] = out_w[u].astype(F32).T.astype(BF16)
        gains[1, u] = jnp.broadcast_to(mix_gain[u : u + 1, :], (128, 128)).T

    def span(r):
        return slice(r * 512, r * 512 + 512)

    def norm_row(u, r):
        nt[:, span(r)] = (normalize(xt[:, span(r)]) * tiled(gains[0, u])).astype(BF16)

    def keep(u, r):
        own = mask[0, r].astype(F32)
        if u == 0:
            return own
        return own * jnp.concatenate([mrow[q : q + 1, :] for q in range(4)], axis=1)

    def panel(u, r, p):
        proj = jnp.dot(wt[u, p * 256 : p * 256 + 256, :], nt[:, span(r)], preferred_element_type=F32)
        return sigmoid(proj[:128]) * proj[128:] * keep(u, r)

    def finish(u, r, recv, k):
        arrived(k, recv)
        unpack(r * 512, 4, recv)
        tri = jnp.concatenate([flat[pl.ds(r * 512 + q, 128, stride=4), :] for q in range(4)], axis=1)
        normed = (normalize(tri) * tiled(gains[1, u])).astype(BF16)
        result = jnp.dot(owt[u], normed, preferred_element_type=F32)
        gate = sigmoid(jnp.dot(gwt[u], nt[:, span(r)], preferred_element_type=F32))
        return xt[:, span(r)] + gate * result

    def part(value, q):
        return value[:, q * 128 : q * 128 + 128]

    for load in loads[:3]:
        load.wait()
    prepare(0)
    for r in range(4):
        flat[pl.ds(r * 512, 512), :] = pair[r].astype(F32)
    for r in range(4):
        for q in range(4):
            at = (r * 4 + q) * 128
            xt[:, at : at + 128] = flat[pl.ds(r * 512 + q, 128, stride=4), :].T
    for r in range(4):
        norm_row(0, r)
        value = panel(0, r, 1)
        for q in range(4):
            flat[pl.ds(2048 + r * 4 + q, 128, stride=16), :] = part(value, q)
    pack(2048, 16, r0_send)

    lane = lax.broadcasted_iota(jnp.int32, (1, 128), 1)
    row = jnp.zeros((1, 128), F32)
    for r in range(4):
        row = jnp.where(lane == r, mask[0, r].astype(F32), row)
    msend[...] = row

    pl.semaphore_wait(barrier, ND - 1)
    exchange(R0, r0_send, r0_recv)
    for r in range(4):
        value = panel(0, r, 0)
        for q in range(4):
            flat[pl.ds(r * 512 + q, 128, stride=4), :] = part(value, q)
        pack(r * 512, 4, l0_send.at[r])
        exchange(L0 + r, l0_send.at[r], l0_recv.at[r])
        if r == 0:
            to_all(
                lambda peer: pltpu.make_async_remote_copy(
                    msend, mrecv.at[me], ssem.at[MASK], rsem.at[MASK], device_id=(peer,), device_id_type=MESH
                ).start()
            )
            mrecv[me] = msend[...]
    for load in loads[3:]:
        load.wait()
    prepare(1)
    prepare_late(0)
    prepare_late(1)

    arrived(MASK, mrecv)
    mrow[...] = mrecv[...].reshape(128, 128).T[0:8]
    arrived(R0, r0_recv)
    unpack(0, 16, r0_recv)
    for r in range(4):
        for q in range(4):
            block = flat[pl.ds(r * 4 + q, 128, stride=16), :]
            mat_b[r * 128 : r * 128 + 128, q * 128 : q * 128 + 128] = block.astype(BF16)
    for r in range(4):
        arrived(L0 + r, l0_recv.at[r])
        unpack(r * 512, 4, l0_recv.at[r])
        for q in range(4):
            block = flat[pl.ds(r * 512 + q, 128, stride=4), :] * mrow[q : q + 1, :]
            mat_a[r, :, q * 128 : q * 128 + 128] = block.astype(BF16)
        tri = lax.dot_general(mat_a[r], mat_b[...], (((1,), (1,)), ((), ())), preferred_element_type=F32)
        for q in range(4):
            flat[pl.ds(2048 + r * 512 + q, 128, stride=4), :] = part(tri, q)
        pack(2048 + r * 512, 4, t0_send.at[r])
        exchange(T0 + r, t0_send.at[r], t0_recv.at[r])

    for r in range(4):
        xt[:, span(r)] = finish(0, r, t0_recv.at[r], T0 + r).astype(BF16).astype(F32)
        norm_row(1, r)
        value = panel(1, r, 1)
        for q in range(4):
            flat[pl.ds(r * 512 + q, 128, stride=4), :] = part(value, q)
        pack(r * 512, 4, r1_send.at[r])
        exchange(R1 + r, r1_send.at[r], r1_recv.at[r])
        value = panel(1, r, 0)
        for q in range(4):
            flat[pl.ds(2048 + q * 512 + r, 128, stride=4), :] = part(value, q)
    for q in range(4):
        pack(2048 + q * 512, 4, l1_send.at[q])
        exchange(L1 + q, l1_send.at[q], l1_recv.at[q])

    for r in range(4):
        arrived(R1 + r, r1_recv.at[r])
        unpack(r * 512, 4, r1_recv.at[r])
        for q in range(4):
            block = flat[pl.ds(r * 512 + q, 128, stride=4), :]
            mat_b[r * 128 : r * 128 + 128, q * 128 : q * 128 + 128] = block.astype(BF16)
    for q in range(4):
        arrived(L1 + q, l1_recv.at[q])
        unpack(q * 512, 4, l1_recv.at[q])
        for r in range(4):
            block = flat[pl.ds(q * 512 + r, 128, stride=4), :]
            mat_a[q, :, r * 128 : r * 128 + 128] = block.T.astype(BF16)
        tri = jnp.dot(mat_a[q], mat_b[...], preferred_element_type=F32)
        for t in range(4):
            flat[pl.ds(2048 + q * 512 + t, 128, stride=4), :] = part(tri, t)
        pack(2048 + q * 512, 4, t1_send.at[q])
        exchange(T1 + q, t1_send.at[q], t1_recv.at[q])

    stores = []
    for r in range(4):
        value = finish(1, r, t1_recv.at[r], T1 + r)
        for q in range(4):
            flat[pl.ds(2048 + r * 512 + q, 128, stride=4), :] = part(value, q).T
        pair[r] = flat[pl.ds(2048 + r * 512, 512), :].astype(BF16)
        stores.append(pltpu.make_async_copy(pair.at[r], out_h.at[r], isem.at[r]))
        stores[-1].start()
    sent(MASK, mrecv)
    sent(R0, r0_send)
    for k, src in ((L0, l0_send), (T0, t0_send), (R1, r1_send), (L1, l1_send), (T1, t1_send)):
        for r in range(4):
            sent(k + r, src.at[r])
    for store in stores:
        store.wait()


def body(pair, residue_mask, norm_gain, proj_weight, gate_weight, mix_gain, out_weight):
    hbm = pl.BlockSpec(memory_space=pltpu.HBM)
    chunks = [pltpu.VMEM((4, ND, 4, 128), BF16)]
    return pl.pallas_call(
        kernel,
        out_shape=jax.ShapeDtypeStruct((4, 512, 128), BF16),
        in_specs=[hbm, pl.BlockSpec(memory_space=pltpu.SMEM)] + [hbm] * 5,
        out_specs=hbm,
        scratch_shapes=[
            pltpu.VMEM((4, 512, 128), BF16),
            pltpu.VMEM((2, 128), F32),
            pltpu.VMEM((2, 128, 512), BF16),
            pltpu.VMEM((2, 128, 128), BF16),
            pltpu.VMEM((2, 128), F32),
            pltpu.VMEM((2, 128, 128), BF16),
            pltpu.SemaphoreType.DMA((6,)),
            pltpu.VMEM((128, 2048), F32),
            pltpu.VMEM((128, 2048), BF16),
            pltpu.VMEM((2, 512, 128), BF16),
            pltpu.VMEM((2, 128, 128), BF16),
            pltpu.VMEM((2, 128, 128), BF16),
            pltpu.VMEM((2, 2, 128, 128), F32),
            pltpu.VMEM((4096, 128), F32),
            pltpu.VMEM((4, 128, 512), BF16),
            pltpu.VMEM((512, 512), BF16),
            pltpu.VMEM((1, 128), F32),
            pltpu.VMEM((ND, 1, 128), F32),
            pltpu.VMEM((8, 128), F32),
        ]
        + [pltpu.VMEM((ND, 16, 128), BF16)] * 2
        + chunks * 10
        + [pltpu.SemaphoreType.DMA((KINDS,))] * 2,
        compiler_params=pltpu.CompilerParams(
            collective_id=0, has_side_effects=True, vmem_limit_bytes=67_043_328
        ),
    )(pair, residue_mask.reshape(1, 4), norm_gain, proj_weight, gate_weight, mix_gain, out_weight)


def solution(mesh):
    in_specs = (P("dap", None, None), P("dap"), P(), P(), P(), P(), P())
    return jax.shard_map(body, mesh=mesh, in_specs=in_specs, out_specs=P("dap", None, None), check_vma=False)
```

```python
import jax
import jax.numpy as jnp
from jax import lax
from jax.experimental import pallas as pl
from jax.experimental.pallas import tpu as pltpu
from jax.sharding import PartitionSpec as P

EPS = 1e-05
ND = 128
MESH = pl.DeviceIdType.MESH
F32 = jnp.float32
BF16 = jnp.bfloat16
R0, L0, T0, R1, L1, T1, KINDS = 0, 1, 5, 9, 11, 15, 19
MASKED = 2.0**100


def sigmoid(v):
    return 0.5 * jnp.tanh(0.5 * v) + 0.5


def normalize(v):
    center = v - jnp.mean(v, axis=0, keepdims=True)
    spread = jnp.mean(center * center, axis=0, keepdims=True)
    return center * lax.rsqrt(spread + EPS)


def tiled(column):
    return jnp.concatenate([column] * 4, axis=1)


def offset_order():
    offs = [(a, b, c, d) for a in range(4) for b in range(4) for c in range(4) for d in range(2)][1:]
    offs.sort(key=lambda o: -sum(min(v, 4 - v) for v in o[:3]))
    groups = {}
    for o in offs:
        key = next(((a, o[a]) for a in range(3) if o[a]), (3, 0))
        groups.setdefault(key, []).append(o)
    timed = [((i + 0.5) / len(g), o) for g in groups.values() for i, o in enumerate(g)]
    timed.sort(key=lambda t: t[0])
    return [o for _, o in timed]


ORDER = offset_order()


def kernel(
    pair_h, mask_h, norm_gain_h, proj_w_h, gate_w_h, mix_gain_h, out_w_h, out,
    pair, mask, norm_gain, proj_w, gate_w, mix_gain, out_w, isem,
    xt, nt, wt, gwt, owt, gains, flat, mat_a, mat_b, mrow,
    r0_send, r0_recv, l0_send, l0_recv, t0_send, t0_recv, r1_send, r1_recv, l1_send, l1_recv, t1_send, t1_recv,
    ssem, rsem,
):
    pairs = (
        (pair_h, pair), (proj_w_h, proj_w), (norm_gain_h, norm_gain), (mask_h, mask),
        (gate_w_h, gate_w), (mix_gain_h, mix_gain), (out_w_h, out_w),
    )
    loads = [pltpu.make_async_copy(a, b, isem.at[i]) for i, (a, b) in enumerate(pairs)]
    for load in loads:
        load.start()
    me = lax.axis_index("dap")
    core, z = lax.rem(me, 2), lax.rem(me // 2, 4)
    y, x = lax.rem(me // 8, 4), me // 32
    xs = [lax.rem(x + d, 4) * 32 for d in range(4)]
    ys = [lax.rem(y + d, 4) * 8 for d in range(4)]
    zs = [lax.rem(z + d, 4) * 2 for d in range(4)]
    cs = [lax.rem(core + d, 2) for d in range(2)]
    peers = [xs[a] + ys[b] + zs[c] + cs[d] for a, b, c, d in ORDER]

    def to_all(send_one):
        for peer in peers:
            send_one(peer)

    barrier = pltpu.get_barrier_semaphore()
    to_all(lambda peer: pl.semaphore_signal(barrier, inc=1, device_id=(peer,), device_id_type=MESH))

    def exchange(k, src, dst):
        to_all(
            lambda peer: pltpu.make_async_remote_copy(
                src.at[peer], dst.at[me], ssem.at[k], rsem.at[k], device_id=(peer,), device_id_type=MESH
            ).start()
        )
        dst[me] = src[me]

    def arrived(k, dst):
        part = dst.at[pl.ds(0, ND - 1)]
        pltpu.make_async_copy(part, part, rsem.at[k]).wait()

    def sent(k, src):
        part = src.at[pl.ds(0, ND - 1)]
        pltpu.make_async_copy(part, part, ssem.at[k]).wait()

    def pack(base, rows, dst):
        per = 128 // rows
        for c in range(rows):
            dst[pl.ds(c * per, per)] = flat[pl.ds(base + c * 128, 128), :].astype(BF16).reshape(per, rows, 128)

    def unpack(base, rows, src):
        per = 128 // rows
        for c in range(rows):
            flat[pl.ds(base + c * 128, 128), :] = src[pl.ds(c * per, per)].reshape(128, 128).astype(F32)

    def prepare(u):
        wt[u] = proj_w[u].astype(F32).T.astype(BF16)
        gains[0, u] = jnp.broadcast_to(norm_gain[u : u + 1, :], (128, 128)).T

    def prepare_late(u):
        gwt[u] = gate_w[u].astype(F32).T.astype(BF16)
        owt[u] = out_w[u].astype(F32).T.astype(BF16)
        gains[1, u] = jnp.broadcast_to(mix_gain[u : u + 1, :], (128, 128)).T

    def span(r):
        return slice(r * 512, r * 512 + 512)

    def norm_row(u, r):
        nt[:, span(r)] = (normalize(xt[:, span(r)]) * tiled(gains[0, u])).astype(BF16)

    def keep(u, r):
        own = mask[0, r].astype(F32)
        if u == 0:
            return own
        return own * jnp.concatenate([mrow[q : q + 1, :] for q in range(4)], axis=1)

    def panel(u, r, p):
        proj = jnp.dot(wt[u, p * 256 : p * 256 + 256, :], nt[:, span(r)], preferred_element_type=F32)
        value = sigmoid(proj[:128]) * proj[128:] * keep(u, r)
        if u == 0 and p == 1:
            value = value + (1.0 - mask[0, r].astype(F32)) * MASKED
        return value

    def finish(u, r, recv, k):
        arrived(k, recv)
        unpack(r * 512, 4, recv)
        tri = jnp.concatenate([flat[pl.ds(r * 512 + q, 128, stride=4), :] for q in range(4)], axis=1)
        normed = (normalize(tri) * tiled(gains[1, u])).astype(BF16)
        result = jnp.dot(owt[u], normed, preferred_element_type=F32)
        gate = sigmoid(jnp.dot(gwt[u], nt[:, span(r)], preferred_element_type=F32))
        return xt[:, span(r)] + gate * result

    def part(value, q):
        return value[:, q * 128 : q * 128 + 128]

    for load in loads[:4]:
        load.wait()
    prepare(0)
    for r in range(4):
        flat[pl.ds(r * 512, 512), :] = pair[r].astype(F32)
    for r in range(4):
        for q in range(4):
            at = (r * 4 + q) * 128
            xt[:, at : at + 128] = flat[pl.ds(r * 512 + q, 128, stride=4), :].T
    for r in range(4):
        norm_row(0, r)
        value = panel(0, r, 1)
        for q in range(4):
            flat[pl.ds(2048 + r * 4 + q, 128, stride=16), :] = part(value, q)
    pack(2048, 16, r0_send)

    pl.semaphore_wait(barrier, ND - 1)
    exchange(R0, r0_send, r0_recv)
    for r in range(4):
        value = panel(0, r, 0)
        for q in range(4):
            flat[pl.ds(r * 512 + q, 128, stride=4), :] = part(value, q)
        pack(r * 512, 4, l0_send.at[r])
        exchange(L0 + r, l0_send.at[r], l0_recv.at[r])
    for load in loads[4:]:
        load.wait()
    prepare(1)
    prepare_late(0)
    prepare_late(1)

    arrived(R0, r0_recv)
    unpack(0, 16, r0_recv)
    for r in range(4):
        for q in range(4):
            block = flat[pl.ds(r * 4 + q, 128, stride=16), :]
            if q == 0:
                mrow[r : r + 1, :] = jnp.where(block.T[0:1] > 0.5 * MASKED, 0.0, 1.0)
            block = jnp.where(block > 0.5 * MASKED, 0.0, block)
            mat_b[r * 128 : r * 128 + 128, q * 128 : q * 128 + 128] = block.astype(BF16)
    for r in range(4):
        arrived(L0 + r, l0_recv.at[r])
        unpack(r * 512, 4, l0_recv.at[r])
        for q in range(4):
            block = flat[pl.ds(r * 512 + q, 128, stride=4), :] * mrow[q : q + 1, :]
            mat_a[r, :, q * 128 : q * 128 + 128] = block.astype(BF16)
        tri = lax.dot_general(mat_a[r], mat_b[...], (((1,), (1,)), ((), ())), preferred_element_type=F32)
        for q in range(4):
            flat[pl.ds(2048 + r * 512 + q, 128, stride=4), :] = part(tri, q)
        pack(2048 + r * 512, 4, t0_send.at[r])
        exchange(T0 + r, t0_send.at[r], t0_recv.at[r])

    for g in range(2):
        for r in (2 * g, 2 * g + 1):
            xt[:, span(r)] = finish(0, r, t0_recv.at[r], T0 + r).astype(BF16).astype(F32)
            norm_row(1, r)
            value = panel(1, r, 1)
            for q in range(4):
                flat[pl.ds(4096 + g * 1024 + (r - 2 * g) * 4 + q, 128, stride=8), :] = part(value, q)
        pack(4096 + g * 1024, 8, r1_send.at[g])
        exchange(R1 + g, r1_send.at[g], r1_recv.at[g])
        for r in (2 * g, 2 * g + 1):
            value = panel(1, r, 0)
            for q in range(4):
                flat[pl.ds(2048 + q * 512 + r, 128, stride=4), :] = part(value, q)
    for q in range(4):
        pack(2048 + q * 512, 4, l1_send.at[q])
        exchange(L1 + q, l1_send.at[q], l1_recv.at[q])

    for g in range(2):
        arrived(R1 + g, r1_recv.at[g])
        unpack(g * 1024, 8, r1_recv.at[g])
        for r in (2 * g, 2 * g + 1):
            for q in range(4):
                block = flat[pl.ds(g * 1024 + (r - 2 * g) * 4 + q, 128, stride=8), :]
                mat_b[r * 128 : r * 128 + 128, q * 128 : q * 128 + 128] = block.astype(BF16)
    for q in range(4):
        arrived(L1 + q, l1_recv.at[q])
        unpack(q * 512, 4, l1_recv.at[q])
        for r in range(4):
            block = flat[pl.ds(q * 512 + r, 128, stride=4), :]
            mat_a[q, :, r * 128 : r * 128 + 128] = block.T.astype(BF16)
        tri = jnp.dot(mat_a[q], mat_b[...], preferred_element_type=F32)
        for t in range(4):
            flat[pl.ds(2048 + q * 512 + t, 128, stride=4), :] = part(tri, t)
        pack(2048 + q * 512, 4, t1_send.at[q])
        exchange(T1 + q, t1_send.at[q], t1_recv.at[q])

    for r in range(4):
        value = finish(1, r, t1_recv.at[r], T1 + r)
        for q in range(4):
            flat[pl.ds(2048 + r * 512 + q, 128, stride=4), :] = part(value, q).T
        out[r] = flat[pl.ds(2048 + r * 512, 512), :].astype(BF16)
    sent(R0, r0_send)
    for k, src, parts in ((L0, l0_send, 4), (T0, t0_send, 4), (R1, r1_send, 2), (L1, l1_send, 4), (T1, t1_send, 4)):
        for r in range(parts):
            sent(k + r, src.at[r])


def at_hbm(a):
    return pltpu.with_memory_space_constraint(a, pltpu.HBM)


def body(*args):
    hbm = pl.BlockSpec(memory_space=pltpu.HBM)
    chunks = [pltpu.VMEM((4, ND, 4, 128), BF16)]
    return pl.pallas_call(
        kernel,
        out_shape=pltpu.VMEM((4, 512, 128), BF16),
        in_specs=[hbm] * 7,
        out_specs=pl.BlockSpec(memory_space=pltpu.VMEM),
        scratch_shapes=[
            pltpu.VMEM((4, 512, 128), BF16),
            pltpu.SMEM((1, 4), jnp.int32),
            pltpu.VMEM((2, 128), F32),
            pltpu.VMEM((2, 128, 512), BF16),
            pltpu.VMEM((2, 128, 128), BF16),
            pltpu.VMEM((2, 128), F32),
            pltpu.VMEM((2, 128, 128), BF16),
            pltpu.SemaphoreType.DMA((7,)),
            pltpu.VMEM((128, 2048), F32),
            pltpu.VMEM((128, 2048), BF16),
            pltpu.VMEM((2, 512, 128), BF16),
            pltpu.VMEM((2, 128, 128), BF16),
            pltpu.VMEM((2, 128, 128), BF16),
            pltpu.VMEM((2, 2, 128, 128), F32),
            pltpu.VMEM((6144, 128), F32),
            pltpu.VMEM((4, 128, 512), BF16),
            pltpu.VMEM((512, 512), BF16),
            pltpu.VMEM((8, 128), F32),
        ]
        + [pltpu.VMEM((ND, 16, 128), BF16)] * 2
        + chunks * 4
        + [pltpu.VMEM((2, ND, 8, 128), BF16)] * 2
        + chunks * 4
        + [pltpu.SemaphoreType.DMA((KINDS,))] * 2,
        compiler_params=pltpu.CompilerParams(
            collective_id=0, has_side_effects=True, vmem_limit_bytes=48 << 20
        ),
    )(*(at_hbm(a if a.ndim > 1 else a.reshape(1, 4)) for a in args))


def solution(mesh):
    in_specs = (P("dap", None, None), P("dap"), P(), P(), P(), P(), P())
    return jax.shard_map(body, mesh=mesh, in_specs=in_specs, out_specs=P("dap", None, None), check_vma=False)
```

```python
import jax
import jax.numpy as jnp
from jax import lax
from jax.experimental import pallas as pl
from jax.experimental.pallas import tpu as pltpu
from jax.sharding import PartitionSpec as P

EPS = 1e-05
ND = 128
MESH = pl.DeviceIdType.MESH
F32 = jnp.float32
BF16 = jnp.bfloat16
R0, L0, T0, R1, L1, T1, KINDS = 0, 2, 6, 10, 14, 18, 22
R1_ROWS = ((0,), (1,), (2,), (3,))
MASKED = 2.0**100


def sigmoid(v):
    return 0.5 * jnp.tanh(0.5 * v) + 0.5


def normalize(v):
    center = v - jnp.mean(v, axis=0, keepdims=True)
    spread = jnp.mean(center * center, axis=0, keepdims=True)
    return center * lax.rsqrt(spread + EPS)


def tiled(column):
    return jnp.concatenate([column] * 4, axis=1)


def offset_order():
    offs = [(a, b, c, d) for a in range(4) for b in range(4) for c in range(4) for d in range(2)][1:]
    offs.sort(key=lambda o: -sum(min(v, 4 - v) for v in o[:3]))
    groups = {}
    for o in offs:
        key = next(((a, o[a]) for a in range(3) if o[a]), (3, 0))
        groups.setdefault(key, []).append(o)
    timed = [((i + 0.5) / len(g), o) for g in groups.values() for i, o in enumerate(g)]
    timed.sort(key=lambda t: t[0])
    return [o for _, o in timed]


ORDER = offset_order()


def kernel(
    pair_h, mask_h, norm_gain_h, proj_w_h, gate_w_h, mix_gain_h, out_w_h, out,
    pair, mask, norm_gain, proj_w, gate_w, mix_gain, out_w, isem,
    xt, nt, gates, wt, gwt, owt, gains, flat, mat_a, mat_b, mrow,
    r0_send, r0_recv, l0_send, l0_recv, t0_send, t0_recv, r1_send, r1_recv, r1_send2, r1_recv2, l1_send, l1_recv, t1_send, t1_recv,
    ssem, rsem,
):
    pairs = (
        (pair_h, pair), (proj_w_h, proj_w), (norm_gain_h, norm_gain), (mask_h, mask),
        (gate_w_h, gate_w), (mix_gain_h, mix_gain), (out_w_h, out_w),
    )
    loads = [pltpu.make_async_copy(a, b, isem.at[i]) for i, (a, b) in enumerate(pairs)]
    for load in loads:
        load.start()
    me = lax.axis_index("dap")
    core, z = lax.rem(me, 2), lax.rem(me // 2, 4)
    y, x = lax.rem(me // 8, 4), me // 32
    xs = [lax.rem(x + d, 4) * 32 for d in range(4)]
    ys = [lax.rem(y + d, 4) * 8 for d in range(4)]
    zs = [lax.rem(z + d, 4) * 2 for d in range(4)]
    cs = [lax.rem(core + d, 2) for d in range(2)]
    peers = [xs[a] + ys[b] + zs[c] + cs[d] for a, b, c, d in ORDER]

    def to_all(send_one):
        for peer in peers:
            send_one(peer)

    barrier = pltpu.get_barrier_semaphore()
    to_all(lambda peer: pl.semaphore_signal(barrier, inc=1, device_id=(peer,), device_id_type=MESH))

    def exchange(k, src, dst):
        to_all(
            lambda peer: pltpu.make_async_remote_copy(
                src.at[peer], dst.at[me], ssem.at[k], rsem.at[k], device_id=(peer,), device_id_type=MESH
            ).start()
        )
        dst[me] = src[me]

    def arrived(k, dst):
        part = dst.at[pl.ds(0, ND - 1)]
        pltpu.make_async_copy(part, part, rsem.at[k]).wait()

    def sent(k, src):
        part = src.at[pl.ds(0, ND - 1)]
        pltpu.make_async_copy(part, part, ssem.at[k]).wait()

    def pack(base, rows, dst):
        per = 128 // rows
        for c in range(rows):
            dst[pl.ds(c * per, per)] = flat[pl.ds(base + c * 128, 128), :].astype(BF16).reshape(per, rows, 128)

    def unpack(base, rows, src):
        per = 128 // rows
        for c in range(rows):
            flat[pl.ds(base + c * 128, 128), :] = src[pl.ds(c * per, per)].reshape(128, 128).astype(F32)

    def prepare(u):
        wt[u] = proj_w[u].astype(F32).T.astype(BF16)
        gains[0, u] = jnp.broadcast_to(norm_gain[u : u + 1, :], (128, 128)).T

    def prepare_late(u):
        gwt[u] = gate_w[u].astype(F32).T.astype(BF16)
        owt[u] = out_w[u].astype(F32).T.astype(BF16)
        gains[1, u] = jnp.broadcast_to(mix_gain[u : u + 1, :], (128, 128)).T

    def span(r):
        return slice(r * 512, r * 512 + 512)

    def norm_row(u, r):
        nt[:, span(r)] = (normalize(xt[:, span(r)]) * tiled(gains[0, u])).astype(BF16)

    def keep(u, r):
        own = mask[0, r].astype(F32)
        if u == 0:
            return own
        return own * jnp.concatenate([mrow[q : q + 1, :] for q in range(4)], axis=1)

    def panel(u, r, p):
        proj = jnp.dot(wt[u, p * 256 : p * 256 + 256, :], nt[:, span(r)], preferred_element_type=F32)
        value = sigmoid(proj[:128]) * proj[128:] * keep(u, r)
        if u == 0 and p == 1:
            value = value + (1.0 - mask[0, r].astype(F32)) * MASKED
        return value

    def finish(u, r, recv, k):
        arrived(k, recv)
        unpack(r * 512, 4, recv)
        tri = jnp.concatenate([flat[pl.ds(r * 512 + q, 128, stride=4), :] for q in range(4)], axis=1)
        normed = (normalize(tri) * tiled(gains[1, u])).astype(BF16)
        result = jnp.dot(owt[u], normed, preferred_element_type=F32)
        return xt[:, span(r)] + gates[:, span(r)] * result

    def gate_row(u, r):
        gates[:, span(r)] = sigmoid(jnp.dot(gwt[u], nt[:, span(r)], preferred_element_type=F32))

    def part(value, q):
        return value[:, q * 128 : q * 128 + 128]

    for load in loads[:4]:
        load.wait()
    prepare(0)
    for r in range(4):
        flat[pl.ds(r * 512, 512), :] = pair[r].astype(F32)
    for r in range(4):
        for q in range(4):
            at = (r * 4 + q) * 128
            xt[:, at : at + 128] = flat[pl.ds(r * 512 + q, 128, stride=4), :].T
    for g in range(2):
        for r in (2 * g, 2 * g + 1):
            norm_row(0, r)
            value = panel(0, r, 1)
            for q in range(4):
                flat[pl.ds(2048 + g * 1024 + (r - 2 * g) * 4 + q, 128, stride=8), :] = part(value, q)
        pack(2048 + g * 1024, 8, r0_send.at[g])
        if g == 0:
            pl.semaphore_wait(barrier, ND - 1)
        exchange(R0 + g, r0_send.at[g], r0_recv.at[g])
    for r in range(4):
        value = panel(0, r, 0)
        for q in range(4):
            flat[pl.ds(r * 512 + q, 128, stride=4), :] = part(value, q)
        pack(r * 512, 4, l0_send.at[r])
        exchange(L0 + r, l0_send.at[r], l0_recv.at[r])
    for load in loads[4:]:
        load.wait()
    prepare(1)
    prepare_late(0)
    prepare_late(1)
    for r in range(4):
        gate_row(0, r)

    for g in range(2):
        arrived(R0 + g, r0_recv.at[g])
        unpack(g * 1024, 8, r0_recv.at[g])
        for r in (2 * g, 2 * g + 1):
            for q in range(4):
                block = flat[pl.ds(g * 1024 + (r - 2 * g) * 4 + q, 128, stride=8), :]
                if q == 0:
                    mrow[r : r + 1, :] = jnp.where(block.T[0:1] > 0.5 * MASKED, 0.0, 1.0)
                block = jnp.where(block > 0.5 * MASKED, 0.0, block)
                mat_b[r * 128 : r * 128 + 128, q * 128 : q * 128 + 128] = block.astype(BF16)
    for r in range(4):
        arrived(L0 + r, l0_recv.at[r])
        unpack(r * 512, 4, l0_recv.at[r])
        for q in range(4):
            block = flat[pl.ds(r * 512 + q, 128, stride=4), :] * mrow[q : q + 1, :]
            mat_a[r, :, q * 128 : q * 128 + 128] = block.astype(BF16)
        tri = lax.dot_general(mat_a[r], mat_b[...], (((1,), (1,)), ((), ())), preferred_element_type=F32)
        for q in range(4):
            flat[pl.ds(2048 + r * 512 + q, 128, stride=4), :] = part(tri, q)
        pack(2048 + r * 512, 4, t0_send.at[r])
        exchange(T0 + r, t0_send.at[r], t0_recv.at[r])

    def left_row(r):
        value = panel(1, r, 0)
        for q in range(4):
            flat[pl.ds(2048 + q * 512 + r, 128, stride=4), :] = part(value, q)

    r1 = [(r1_send.at[i], r1_recv.at[i]) if len(rows) == 1 else (r1_send2, r1_recv2) for i, rows in enumerate(R1_ROWS)]
    for i, rows in enumerate(R1_ROWS):
        n = len(rows)
        for r in rows:
            xt[:, span(r)] = finish(0, r, t0_recv.at[r], T0 + r).astype(BF16).astype(F32)
            norm_row(1, r)
            value = panel(1, r, 1)
            for q in range(4):
                flat[pl.ds(4096 + rows[0] * 512 + (r - rows[0]) * 4 + q, 128, stride=4 * n), :] = part(value, q)
        pack(4096 + rows[0] * 512, 4 * n, r1[i][0])
        exchange(R1 + i, *r1[i])
    for r in range(4):
        left_row(r)
    for q in range(4):
        pack(2048 + q * 512, 4, l1_send.at[q])
        exchange(L1 + q, l1_send.at[q], l1_recv.at[q])

    for r in range(4):
        gate_row(1, r)

    for i, rows in enumerate(R1_ROWS):
        n = len(rows)
        arrived(R1 + i, r1[i][1])
        unpack(rows[0] * 512, 4 * n, r1[i][1])
        for r in rows:
            for q in range(4):
                block = flat[pl.ds(rows[0] * 512 + (r - rows[0]) * 4 + q, 128, stride=4 * n), :]
                mat_b[r * 128 : r * 128 + 128, q * 128 : q * 128 + 128] = block.astype(BF16)
    for q in range(4):
        arrived(L1 + q, l1_recv.at[q])
        unpack(q * 512, 4, l1_recv.at[q])
        for r in range(4):
            block = flat[pl.ds(q * 512 + r, 128, stride=4), :]
            mat_a[q, :, r * 128 : r * 128 + 128] = block.T.astype(BF16)
        tri = jnp.dot(mat_a[q], mat_b[...], preferred_element_type=F32)
        for t in range(4):
            flat[pl.ds(2048 + q * 512 + t, 128, stride=4), :] = part(tri, t)
        pack(2048 + q * 512, 4, t1_send.at[q])
        exchange(T1 + q, t1_send.at[q], t1_recv.at[q])

    for r in range(4):
        value = finish(1, r, t1_recv.at[r], T1 + r)
        for q in range(4):
            flat[pl.ds(2048 + r * 512 + q, 128, stride=4), :] = part(value, q).T
        out[r] = flat[pl.ds(2048 + r * 512, 512), :].astype(BF16)
    for i in range(len(R1_ROWS)):
        sent(R1 + i, r1[i][0])
    for k, src, parts in (
        (R0, r0_send, 2),
        (L0, l0_send, 4),
        (T0, t0_send, 4),
        (L1, l1_send, 4),
        (T1, t1_send, 4),
    ):
        for r in range(parts):
            sent(k + r, src.at[r])


def at_hbm(a):
    return pltpu.with_memory_space_constraint(a, pltpu.HBM)


def body(*args):
    hbm = pl.BlockSpec(memory_space=pltpu.HBM)
    chunks = [pltpu.VMEM((4, ND, 4, 128), BF16)]
    return pl.pallas_call(
        kernel,
        out_shape=pltpu.VMEM((4, 512, 128), BF16),
        in_specs=[hbm] * 7,
        out_specs=pl.BlockSpec(memory_space=pltpu.VMEM),
        scratch_shapes=[
            pltpu.VMEM((4, 512, 128), BF16),
            pltpu.SMEM((1, 4), jnp.int32),
            pltpu.VMEM((2, 128), F32),
            pltpu.VMEM((2, 128, 512), BF16),
            pltpu.VMEM((2, 128, 128), BF16),
            pltpu.VMEM((2, 128), F32),
            pltpu.VMEM((2, 128, 128), BF16),
            pltpu.SemaphoreType.DMA((7,)),
            pltpu.VMEM((128, 2048), F32),
            pltpu.VMEM((128, 2048), BF16),
            pltpu.VMEM((128, 2048), F32),
            pltpu.VMEM((2, 512, 128), BF16),
            pltpu.VMEM((2, 128, 128), BF16),
            pltpu.VMEM((2, 128, 128), BF16),
            pltpu.VMEM((2, 2, 128, 128), F32),
            pltpu.VMEM((6144, 128), F32),
            pltpu.VMEM((4, 128, 512), BF16),
            pltpu.VMEM((512, 512), BF16),
            pltpu.VMEM((8, 128), F32),
        ]
        + [pltpu.VMEM((2, ND, 8, 128), BF16)] * 2
        + chunks * 6
        + [pltpu.VMEM((ND, 8, 128), BF16)] * 2
        + chunks * 4
        + [pltpu.SemaphoreType.DMA((KINDS,))] * 2,
        compiler_params=pltpu.CompilerParams(
            collective_id=0, has_side_effects=True, vmem_limit_bytes=48 << 20
        ),
    )(*(at_hbm(a if a.ndim > 1 else a.reshape(1, 4)) for a in args))


def solution(mesh):
    in_specs = (P("dap", None, None), P("dap"), P(), P(), P(), P(), P())
    return jax.shard_map(body, mesh=mesh, in_specs=in_specs, out_specs=P("dap", None, None), check_vma=False)
```

```python
import jax
import jax.numpy as jnp
from jax import lax
from jax.experimental import pallas as pl
from jax.experimental.pallas import tpu as pltpu
from jax.sharding import PartitionSpec as P

EPS = 1e-05
ND = 128
MESH = pl.DeviceIdType.MESH
F32 = jnp.float32
BF16 = jnp.bfloat16
R0, L0, T0, R1, L1, T1, KINDS = 0, 4, 8, 12, 16, 20, 24
MASKED = 2.0**100


def sigmoid(v):
    return 0.5 * jnp.tanh(0.5 * v) + 0.5


def normalize(v):
    center = v - jnp.mean(v, axis=0, keepdims=True)
    spread = jnp.mean(center * center, axis=0, keepdims=True)
    return center * lax.rsqrt(spread + EPS)


def tiled(column):
    return jnp.concatenate([column] * 4, axis=1)


def offset_order():
    offs = [(a, b, c, d) for a in range(4) for b in range(4) for c in range(4) for d in range(2)][1:]
    offs.sort(key=lambda o: -sum(min(v, 4 - v) for v in o[:3]))
    groups = {}
    for o in offs:
        key = next(((a, o[a]) for a in range(3) if o[a]), (3, 0))
        groups.setdefault(key, []).append(o)
    timed = [((i + 0.5) / len(g), o) for g in groups.values() for i, o in enumerate(g)]
    timed.sort(key=lambda t: t[0])
    return [o for _, o in timed]


ORDER = offset_order()


def kernel(
    pair_h, mask_h, norm_gain_h, proj_w_h, gate_w_h, mix_gain_h, out_w_h, out,
    pair, mask, norm_gain, proj_w, gate_w, mix_gain, out_w, isem,
    xt, nt, gates, wt, gwt, owt, gains, flat, mat_a, mat_b, mrow,
    r0_send, r0_recv, l0_send, l0_recv, t0_send, t0_recv, r1_send, r1_recv, l1_send, l1_recv, t1_send, t1_recv,
    ssem, rsem,
):
    pairs = (
        (pair_h, pair), (proj_w_h, proj_w), (norm_gain_h, norm_gain), (mask_h, mask),
        (gate_w_h, gate_w), (mix_gain_h, mix_gain), (out_w_h, out_w),
    )
    loads = [pltpu.make_async_copy(a, b, isem.at[i]) for i, (a, b) in enumerate(pairs)]
    for load in loads:
        load.start()
    me = lax.axis_index("dap")
    core, z = lax.rem(me, 2), lax.rem(me // 2, 4)
    y, x = lax.rem(me // 8, 4), me // 32
    xs = [lax.rem(x + d, 4) * 32 for d in range(4)]
    ys = [lax.rem(y + d, 4) * 8 for d in range(4)]
    zs = [lax.rem(z + d, 4) * 2 for d in range(4)]
    cs = [lax.rem(core + d, 2) for d in range(2)]
    peers = [xs[a] + ys[b] + zs[c] + cs[d] for a, b, c, d in ORDER]

    def to_all(send_one):
        for peer in peers:
            send_one(peer)

    barrier = pltpu.get_barrier_semaphore()
    to_all(lambda peer: pl.semaphore_signal(barrier, inc=1, device_id=(peer,), device_id_type=MESH))

    def exchange(k, src, dst):
        to_all(
            lambda peer: pltpu.make_async_remote_copy(
                src.at[peer], dst.at[me], ssem.at[k], rsem.at[k], device_id=(peer,), device_id_type=MESH
            ).start()
        )
        dst[me] = src[me]

    def arrived(k, dst):
        part = dst.at[pl.ds(0, ND - 1)]
        pltpu.make_async_copy(part, part, rsem.at[k]).wait()

    def sent(k, src):
        part = src.at[pl.ds(0, ND - 1)]
        pltpu.make_async_copy(part, part, ssem.at[k]).wait()

    def pack(base, rows, dst):
        per = 128 // rows
        for c in range(rows):
            dst[pl.ds(c * per, per)] = flat[pl.ds(base + c * 128, 128), :].astype(BF16).reshape(per, rows, 128)

    def unpack(base, rows, src):
        per = 128 // rows
        for c in range(rows):
            flat[pl.ds(base + c * 128, 128), :] = src[pl.ds(c * per, per)].reshape(128, 128).astype(F32)

    def prepare(u):
        wt[u] = proj_w[u].astype(F32).T.astype(BF16)
        gains[0, u] = jnp.broadcast_to(norm_gain[u : u + 1, :], (128, 128)).T

    def prepare_late(u):
        gwt[u] = gate_w[u].astype(F32).T.astype(BF16)
        owt[u] = out_w[u].astype(F32).T.astype(BF16)
        gains[1, u] = jnp.broadcast_to(mix_gain[u : u + 1, :], (128, 128)).T

    def span(r):
        return slice(r * 512, r * 512 + 512)

    def norm_row(u, r):
        nt[:, span(r)] = (normalize(xt[:, span(r)]) * tiled(gains[0, u])).astype(BF16)

    def keep(u, r):
        own = mask[0, r].astype(F32)
        if u == 0:
            return own
        return own * jnp.concatenate([mrow[q : q + 1, :] for q in range(4)], axis=1)

    def panel(u, r, p):
        proj = jnp.dot(wt[u, p * 256 : p * 256 + 256, :], nt[:, span(r)], preferred_element_type=F32)
        value = sigmoid(proj[:128]) * proj[128:] * keep(u, r)
        if u == 0 and p == 1:
            value = value + (1.0 - mask[0, r].astype(F32)) * MASKED
        return value

    def finish(u, r, recv, k):
        arrived(k, recv)
        unpack(r * 512, 4, recv)
        tri = jnp.concatenate([flat[pl.ds(r * 512 + q, 128, stride=4), :] for q in range(4)], axis=1)
        normed = (normalize(tri) * tiled(gains[1, u])).astype(BF16)
        result = jnp.dot(owt[u], normed, preferred_element_type=F32)
        return xt[:, span(r)] + gates[:, span(r)] * result

    def gate_row(u, r):
        gates[:, span(r)] = sigmoid(jnp.dot(gwt[u], nt[:, span(r)], preferred_element_type=F32))

    def part(value, q):
        return value[:, q * 128 : q * 128 + 128]

    for load in loads[:4]:
        load.wait()
    prepare(0)
    for r in range(4):
        flat[pl.ds(r * 512, 512), :] = pair[r].astype(F32)
    for r in range(4):
        for q in range(4):
            at = (r * 4 + q) * 128
            xt[:, at : at + 128] = flat[pl.ds(r * 512 + q, 128, stride=4), :].T
    for r in range(4):
        norm_row(0, r)
        value = panel(0, r, 1)
        for q in range(4):
            flat[pl.ds(2048 + r * 512 + q, 128, stride=4), :] = part(value, q)
        pack(2048 + r * 512, 4, r0_send.at[r])
        if r == 0:
            pl.semaphore_wait(barrier, ND - 1)
        exchange(R0 + r, r0_send.at[r], r0_recv.at[r])
    for r in range(4):
        value = panel(0, r, 0)
        for q in range(4):
            flat[pl.ds(r * 512 + q, 128, stride=4), :] = part(value, q)
        pack(r * 512, 4, l0_send.at[r])
        exchange(L0 + r, l0_send.at[r], l0_recv.at[r])
    for load in loads[4:]:
        load.wait()
    prepare(1)
    prepare_late(0)
    prepare_late(1)
    for r in range(4):
        gate_row(0, r)

    for r in range(4):
        arrived(R0 + r, r0_recv.at[r])
        unpack(r * 512, 4, r0_recv.at[r])
        for q in range(4):
            block = flat[pl.ds(r * 512 + q, 128, stride=4), :]
            if q == 0:
                mrow[r : r + 1, :] = jnp.where(block.T[0:1] > 0.5 * MASKED, 0.0, 1.0)
            block = jnp.where(block > 0.5 * MASKED, 0.0, block)
            mat_b[r * 128 : r * 128 + 128, q * 128 : q * 128 + 128] = block.astype(BF16)
    for r in range(4):
        arrived(L0 + r, l0_recv.at[r])
        unpack(r * 512, 4, l0_recv.at[r])
        for q in range(4):
            block = flat[pl.ds(r * 512 + q, 128, stride=4), :] * mrow[q : q + 1, :]
            mat_a[r, :, q * 128 : q * 128 + 128] = block.astype(BF16)
        tri = lax.dot_general(mat_a[r], mat_b[...], (((1,), (1,)), ((), ())), preferred_element_type=F32)
        for q in range(4):
            flat[pl.ds(2048 + r * 512 + q, 128, stride=4), :] = part(tri, q)
        pack(2048 + r * 512, 4, t0_send.at[r])
        exchange(T0 + r, t0_send.at[r], t0_recv.at[r])

    def left_row(r):
        value = panel(1, r, 0)
        for q in range(4):
            flat[pl.ds(2048 + q * 512 + r, 128, stride=4), :] = part(value, q)

    for r in range(4):
        xt[:, span(r)] = finish(0, r, t0_recv.at[r], T0 + r).astype(BF16).astype(F32)
        norm_row(1, r)
        value = panel(1, r, 1)
        for q in range(4):
            flat[pl.ds(4096 + r * 512 + q, 128, stride=4), :] = part(value, q)
        pack(4096 + r * 512, 4, r1_send.at[r])
        exchange(R1 + r, r1_send.at[r], r1_recv.at[r])
    for r in range(4):
        left_row(r)
    for q in range(4):
        pack(2048 + q * 512, 4, l1_send.at[q])
        exchange(L1 + q, l1_send.at[q], l1_recv.at[q])

    for r in range(4):
        gate_row(1, r)

    for r in range(4):
        arrived(R1 + r, r1_recv.at[r])
        unpack(r * 512, 4, r1_recv.at[r])
        for q in range(4):
            block = flat[pl.ds(r * 512 + q, 128, stride=4), :]
            mat_b[r * 128 : r * 128 + 128, q * 128 : q * 128 + 128] = block.astype(BF16)
    for q in range(4):
        arrived(L1 + q, l1_recv.at[q])
        unpack(q * 512, 4, l1_recv.at[q])
        for r in range(4):
            block = flat[pl.ds(q * 512 + r, 128, stride=4), :]
            mat_a[q, :, r * 128 : r * 128 + 128] = block.T.astype(BF16)
        tri = jnp.dot(mat_a[q], mat_b[...], preferred_element_type=F32)
        for t in range(4):
            flat[pl.ds(2048 + q * 512 + t, 128, stride=4), :] = part(tri, t)
        pack(2048 + q * 512, 4, t1_send.at[q])
        exchange(T1 + q, t1_send.at[q], t1_recv.at[q])

    for r in range(4):
        value = finish(1, r, t1_recv.at[r], T1 + r)
        for q in range(4):
            flat[pl.ds(2048 + r * 512 + q, 128, stride=4), :] = part(value, q).T
        out[r] = flat[pl.ds(2048 + r * 512, 512), :].astype(BF16)
    for k, src, parts in (
        (R0, r0_send, 4),
        (L0, l0_send, 4),
        (T0, t0_send, 4),
        (R1, r1_send, 4),
        (L1, l1_send, 4),
        (T1, t1_send, 4),
    ):
        for r in range(parts):
            sent(k + r, src.at[r])


def at_hbm(a):
    return pltpu.with_memory_space_constraint(a, pltpu.HBM)


def body(*args):
    hbm = pl.BlockSpec(memory_space=pltpu.HBM)
    chunks = [pltpu.VMEM((4, ND, 4, 128), BF16)]
    return pl.pallas_call(
        kernel,
        out_shape=pltpu.VMEM((4, 512, 128), BF16),
        in_specs=[hbm] * 7,
        out_specs=pl.BlockSpec(memory_space=pltpu.VMEM),
        scratch_shapes=[
            pltpu.VMEM((4, 512, 128), BF16),
            pltpu.SMEM((1, 4), jnp.int32),
            pltpu.VMEM((2, 128), F32),
            pltpu.VMEM((2, 128, 512), BF16),
            pltpu.VMEM((2, 128, 128), BF16),
            pltpu.VMEM((2, 128), F32),
            pltpu.VMEM((2, 128, 128), BF16),
            pltpu.SemaphoreType.DMA((7,)),
            pltpu.VMEM((128, 2048), F32),
            pltpu.VMEM((128, 2048), BF16),
            pltpu.VMEM((128, 2048), F32),
            pltpu.VMEM((2, 512, 128), BF16),
            pltpu.VMEM((2, 128, 128), BF16),
            pltpu.VMEM((2, 128, 128), BF16),
            pltpu.VMEM((2, 2, 128, 128), F32),
            pltpu.VMEM((6160, 128), F32),
            pltpu.VMEM((4, 128, 512), BF16),
            pltpu.VMEM((512, 512), BF16),
            pltpu.VMEM((8, 128), F32),
        ]
        + chunks * 12
        + [pltpu.SemaphoreType.DMA((KINDS,))] * 2,
        compiler_params=pltpu.CompilerParams(
            collective_id=0, has_side_effects=True, vmem_limit_bytes=48 << 20
        ),
    )(*(at_hbm(a if a.ndim > 1 else a.reshape(1, 4)) for a in args))


def solution(mesh):
    in_specs = (P("dap", None, None), P("dap"), P(), P(), P(), P(), P())
    return jax.shard_map(body, mesh=mesh, in_specs=in_specs, out_specs=P("dap", None, None), check_vma=False)
```
